256 devices in a mesh: section: 8 (over x, core), ep: 32 (over y, z).
Axes of the slice: x: 4, y: 4, z: 8, core: 2. Of those that a mesh axis runs over, the one named last changes fastest.
Arguments:
- hidden_states: bfloat16 [1536, 6144], P('ep'), may hold values from -6 to 6
- route_experts: int32 [1536, 2], P('ep'), may hold values from 0 to 7, all different within a row; in each aligned block of 48 rows (0 to 47, 48 to 95, ...) at most 24 rows name the same one
- route_weights: float32 [1536, 2], P('ep'), may hold values from 0.05 to 1
- gate_weight: bfloat16 [32, 6144, 2048], P('ep', None, 'section'), may hold values from -0.078125 to 0.078125
- up_weight: bfloat16 [32, 6144, 2048], P('ep', None, 'section'), may hold values from -0.078125 to 0.078125
- down_weight: bfloat16 [32, 2048, 6144], P('ep', 'section'), may hold values from -0.0625 to 0.0625
Outputs:
- layer_out: bfloat16 [1536, 6144], P('ep', 'section')
The draws below stay inside these ranges and needn't reach their ends.
Inputs may be any that keep to these rules, and one draw needn't show every extreme that they name: `route_experts`: each row names two different experts. Among the 48 rows of one ep index no expert is named by more than 24 rows, and in every draw some expert is named by exactly 24 rows of some ep index.
All inputs are finite; a program needn't handle non-finite values.
Results may differ from the reference program's by a relative error of at most 0.015.
Values may be sent and summed in bfloat16 or wider, within the bound.
No kernel may reach another device: no remote copies, remote signals or barrier semaphores. Data moves between devices by JAX's collectives and lax.ppermute only.
A program may use at most 128 MiB of HBM per device.

```python
import math
import jax
import jax.numpy as jnp
import numpy as np
from jax import lax

D = 6144
FF = 8192
EXPERTS = 8
TOK_DEV = 48
TOKENS = 1536
CAP = 24
MEMBERS = 4
N_SECTION = 8
N_EP = 32


def levels(key, extent, pieces, smallest, top_value):
    factor_of, own = 1.0, jax.random.fold_in(key, 6)
    for axis_at, blocks in pieces:
        steps = jnp.exp(jax.random.uniform(jax.random.fold_in(own, axis_at), (blocks,), jnp.float32, smallest / len(pieces), top_value / len(pieces)))
        factor_of = factor_of * jnp.repeat(steps, extent[axis_at] // blocks).reshape([-1 if axis == axis_at else 1 for axis in range(len(extent))])
    return factor_of


def routed_block(own_key, own, number, rows, count, top, most, lean):
    ranking = jax.random.permutation(own_key, count)
    packed, ordinary = portions_of(count, rows * top, most, lean, True), portions_of(count, rows * top, most, lean, False)
    places = jnp.arange(count)

    def named(sizes, turn):
        used = int((sizes > 0).sum())
        fixed = max(1, used // 4)
        passed = fixed + (places - fixed + turn * (used - fixed)) % max(1, count - fixed)
        return jnp.zeros((count,), jnp.int32).at[ranking[jnp.where(places < fixed, places, passed)]].set(jnp.asarray(sizes, jnp.int32))

    sizes = jnp.where(number % 4 == 0, named(packed, number // 4), named(ordinary, number - number // 4 - 1))
    mixed = jax.random.permutation(jax.random.fold_in(own, 3), count)
    donor, receiver = mixed[0:count // 2 * 2:2], mixed[1:count // 2 * 2:2]
    margin = jnp.minimum(sizes[donor] - 1, most - sizes[receiver]) // 2
    margin = jnp.where((donor == ranking[0]) | (receiver == ranking[0]) | (sizes[receiver] == 0), 0, jnp.maximum(margin, 0))
    passed = jax.random.randint(jax.random.fold_in(own, 4), (count // 2,), 0, 1 << 20) % (margin + 1)
    sizes = sizes.at[donor].add(-passed).at[receiver].add(passed)
    items = jnp.searchsorted(jnp.cumsum(sizes), jnp.arange(rows * top), side="right").astype(jnp.int32)
    table = items.reshape(top, rows).T
    table = table[jax.random.permutation(jax.random.fold_in(own, 1), rows)]
    turn = jax.random.randint(jax.random.fold_in(own, 2), (rows, 1), 0, top)
    return jnp.take_along_axis(table, (jnp.arange(top)[None, :] + turn) % top, axis=1)


def portions_of(amount, total, limit, lean, full):
    portions = [(1 << 20) // math.isqrt(rank ** lean) + 1 for rank in range(1, amount + 1)]
    largest = limit if full else min(limit, max(-(-total // amount), total * portions[0] // sum(portions)))
    least = 1 if total - largest >= amount - 1 else 0
    holding, spare = [largest] + [least] * (amount - 1), total - largest - least * (amount - 1)
    while spare > 0:
        candidates = [i for i in range(1, amount) if holding[i] < largest] or [i for i in range(1, amount) if holding[i] < limit]
        pool, budget = sum([portions[i] for i in candidates]), spare
        for i in candidates:
            extra = min(limit - holding[i], max(1, budget * portions[i] // pool), spare)
            holding[i] = holding[i] + extra
            spare = spare - extra
    return np.array(holding)


def gaussian(own_key, shape, spread, limit, cuts=(), held_as=jnp.bfloat16):
    drawn = spread * jax.random.normal(own_key, shape, jnp.float32)
    if cuts:
        drawn = drawn * levels(own_key, shape, cuts, -0.22, 0.18)
    return jnp.clip(drawn, -limit, limit).astype(held_as)


def setup_inputs(seed: int = 0) -> dict:
    streams_of = jax.random.split(jax.random.key(seed), 7)
    hidden_states = gaussian(streams_of[0], (TOKENS, D), 1.0, 6.0, ((0, 32),))
    route_experts_keys = jax.random.split(jax.random.fold_in(streams_of[1], 1), TOKENS // TOK_DEV)
    route_experts_turns = jax.random.permutation(jax.random.fold_in(streams_of[1], 3), TOKENS // TOK_DEV)
    route_experts = jax.vmap(lambda own, number: routed_block(jax.random.fold_in(streams_of[1], 2), own, number, TOK_DEV, EXPERTS, 2, CAP, 2))(route_experts_keys, route_experts_turns).reshape((TOKENS, 2))
    route_weights = jnp.clip(0.05 + 0.95 * jax.random.uniform(streams_of[2], (TOKENS, 2), jnp.float32) ** levels(streams_of[2], (TOKENS, 2), ((0, 32),), -0.2, 0.2), 0.05, 1.0)
    gate_weight = gaussian(streams_of[3], (N_EP, D, FF // MEMBERS), D ** -0.5, 0.078125, ((0, 32), (2, 8)))
    up_weight = gaussian(streams_of[4], (N_EP, D, FF // MEMBERS), D ** -0.5, 0.078125, ((0, 32), (2, 8)))
    down_weight = gaussian(streams_of[5], (N_EP, FF // MEMBERS, D), FF ** -0.5, 0.0625, ((0, 32), (1, 8)))
    return dict(hidden_states=hidden_states, route_experts=route_experts, route_weights=route_weights, gate_weight=gate_weight, up_weight=up_weight, down_weight=down_weight)


def shard_output(slot_rows, gate_block, up_block, down_block):
    gate_value = jnp.dot(slot_rows, gate_block, preferred_element_type=jnp.float32)
    up_value = jnp.dot(slot_rows, up_block, preferred_element_type=jnp.float32)
    hidden = (jax.nn.silu(gate_value) * up_value).astype(jnp.bfloat16)
    return jnp.dot(hidden, down_block, preferred_element_type=jnp.float32).astype(jnp.bfloat16).astype(jnp.float32)


def reference(hidden_states, route_experts, route_weights, gate_weight, up_weight, down_weight):
    members = N_EP // EXPERTS
    capacity = TOK_DEV // 2
    shard_width = gate_weight.shape[2] // N_SECTION
    blocks = route_experts.reshape(N_EP, TOK_DEV * 2)
    labels = jnp.arange(EXPERTS, dtype=jnp.int32)
    one_hot = (blocks[:, :, None] == labels[None, None, :]).astype(jnp.int32)
    earlier = jnp.cumsum(one_hot, axis=1) - one_hot
    slot_index = jnp.sum(earlier * one_hot, axis=2)
    entry = jnp.arange(TOK_DEV * 2, dtype=jnp.int32)
    token_row = jnp.arange(N_EP, dtype=jnp.int32)[:, None] * TOK_DEV + entry[None, :] // 2
    flat_weights = route_weights.reshape(N_EP, TOK_DEV * 2)
    slots = jnp.arange(capacity, dtype=jnp.int32)
    result = jnp.zeros((TOKENS, D), jnp.float32)
    for expert in range(EXPERTS):
        matches = ((blocks[:, None, :] == expert) & (slot_index[:, None, :] == slots[None, :, None])).astype(jnp.int32)
        rows_index = jnp.sum(matches * token_row[:, None, :], axis=2).reshape(-1).astype(jnp.int32)
        weight_slot = jnp.sum(matches.astype(jnp.float32) * flat_weights[:, None, :], axis=2).reshape(-1)
        gathered = hidden_states[rows_index]

        def add_shard(shard, total):
            member = shard // N_SECTION
            section_index = shard % N_SECTION
            block_index = (expert * members + member).astype(jnp.int32)
            offset = (section_index * shard_width).astype(jnp.int32)
            gate_block = lax.dynamic_slice_in_dim(lax.dynamic_index_in_dim(gate_weight, block_index, 0, keepdims=False), offset, shard_width, 1)
            up_block = lax.dynamic_slice_in_dim(lax.dynamic_index_in_dim(up_weight, block_index, 0, keepdims=False), offset, shard_width, 1)
            down_block = lax.dynamic_slice_in_dim(lax.dynamic_index_in_dim(down_weight, block_index, 0, keepdims=False), offset, shard_width, 0)
            return total + shard_output(gathered, gate_block, up_block, down_block)

        total = lax.fori_loop(0, members * N_SECTION, add_shard, jnp.zeros((N_EP * capacity, D), jnp.float32))
        result = result.at[rows_index].add(weight_slot[:, None] * total)
    return result.astype(jnp.bfloat16)
```

```python
import functools

import jax
import jax.numpy as jnp
from jax import lax
from jax.experimental import pallas as pl
from jax.experimental.pallas import tpu as pltpu
from jax.sharding import Mesh
from jax.sharding import PartitionSpec as P

EXPERTS = 8
MEMBERS = 4
X = 4
CHUNKS = ((0, 1), (3, 2))
GATE_ORDER = (0, 1, 3, 2)
DOWN_ORDER = (2, 1, 3, 0)


def shifted(v, axis, n, step):
    return lax.ppermute(v, axis, [((i + step) % n, i) for i in range(n)])


def ffn_kernel(blocks, half, x_ref, *refs):
    pieces = [refs[5 * b : 5 * b + 5] for b in range(blocks)]
    refs = refs[5 * blocks :]
    g0, g1, u0, u1, d0, d1 = refs[:6]
    outs = [refs[6 + 7 * b : 13 + 7 * b] for b in range(blocks)]
    rows_x, ag0, ag1, au0, au1, h0, h1 = refs[6 + 7 * blocks :]
    step = pl.program_id(0)
    rows = 2 * half

    for at, rel in enumerate(GATE_ORDER):

        @pl.when(step == at)
        def _():
            for b in range(blocks):
                own, plus, minus, far0, far1 = pieces[b]
                base = b * rows
                if rel == 2:
                    rows_x[base : base + half, :] = far0[...]
                    rows_x[base + half : base + rows, :] = far1[...]
                else:
                    src = {0: own, 1: plus, 3: minus}[rel]
                    rows_x[base : base + rows, :] = src[...]

    @pl.when(step < 4)
    def _():
        for w, acc in ((g0, ag0), (g1, ag1), (u0, au0), (u1, au1)):
            part = jnp.dot(rows_x[...], w[...], preferred_element_type=jnp.float32)

            @pl.when(step == 0)
            def _():
                acc[...] = part

            @pl.when(step > 0)
            def _():
                acc[...] += part

    @pl.when(step == 3)
    def _():
        for ag, au, h in ((ag0, au0, h0), (ag1, au1, h1)):
            gate = ag[...]
            h[...] = (gate / (1.0 + jnp.exp(-gate)) * au[...]).astype(jnp.bfloat16)

    for at, rel in enumerate(DOWN_ORDER):

        @pl.when(step == 4 + at)
        def _():
            out = jnp.dot(h0[...], d0[...], preferred_element_type=jnp.float32)
            out += jnp.dot(h1[...], d1[...], preferred_element_type=jnp.float32)
            out = out.astype(jnp.bfloat16)
            for b in range(blocks):
                far0, far1, plus0, plus1, minus0, minus1, own = outs[b]
                base = b * rows
                if rel == 0:
                    own[...] = out[base : base + rows, :]
                else:
                    first, second = {2: (far0, far1), 1: (plus0, plus1), 3: (minus0, minus1)}[rel]
                    first[...] = out[base : base + half, :]
                    second[...] = out[base + half : base + rows, :]


def ffn(x_at, pieces, weights):
    blocks = len(pieces)
    rows, width = pieces[0][0].shape
    half = rows // 2
    hidden = weights[0].shape[1]

    def rel_of(order, at):
        rel = order[0]
        for i in range(1, 4):
            rel = jnp.where(at == i, order[i], rel)
        return rel

    def gate_map(s, x_ref):
        return (lax.rem(x_ref[0] + rel_of(GATE_ORDER, jnp.minimum(s, 3)), 4), 0)

    def down_map(s, x_ref):
        return (0, lax.rem(x_ref[0] + rel_of(DOWN_ORDER, jnp.maximum(s - 4, 0)), 4))

    def whole(shape):
        return pl.BlockSpec(shape, lambda s, x_ref: (0, 0), pipeline_mode=pl.Buffered(1))

    flat = [p for block in pieces for p in block]
    out_rows = [half] * 6 + [rows]
    total = blocks * rows
    outs = pl.pallas_call(
        functools.partial(ffn_kernel, blocks, half),
        grid_spec=pltpu.PrefetchScalarGridSpec(
            num_scalar_prefetch=1,
            grid=(8,),
            in_specs=[whole(p.shape) for p in flat]
            + [pl.BlockSpec((width, hidden), gate_map)] * 4
            + [pl.BlockSpec((hidden, width), down_map)] * 2,
            out_specs=[whole((r, width)) for r in out_rows * blocks],
            scratch_shapes=[pltpu.VMEM((total, width), jnp.bfloat16)]
            + [pltpu.VMEM((total, hidden), jnp.float32)] * 4
            + [pltpu.VMEM((total, hidden), jnp.bfloat16)] * 2,
        ),
        out_shape=[jax.ShapeDtypeStruct((r, width), jnp.bfloat16) for r in out_rows * blocks],
        compiler_params=pltpu.CompilerParams(
            dimension_semantics=("arbitrary",), vmem_limit_bytes=32 << 20
        ),
        cost_estimate=pl.CostEstimate(
            flops=2 * total * 4 * width * 2 * hidden * 3,
            bytes_accessed=6 * 4 * width * hidden * 2 + 2 * total * 4 * width * 2,
            transcendentals=total * 2 * hidden,
        ),
        name="ffn",
    )(x_at, *flat, *weights)
    return [outs[7 * b : 7 * b + 7] for b in range(blocks)]


def add(*parts):
    return functools.reduce(jnp.add, [p.astype(jnp.float32) for p in parts]).astype(jnp.bfloat16)


def on_device(hidden_states, route_experts, route_weights, gate_weight, up_weight, down_weight):
    x_index, core = lax.axis_index("x"), lax.axis_index("core")
    tok_rows, features = hidden_states.shape
    capacity = tok_rows // 2
    slots = capacity // 2
    width = features // X
    narrow = width // 2

    own_w = (gate_weight[0], up_weight[0], down_weight[0])
    other_w = [shifted(w, "core", 2, 1) for w in own_w]
    weights = [own_w[0], other_w[0], own_w[1], other_w[1], own_w[2], other_w[2]]

    chosen = route_experts.reshape(-1)
    one_hot = (chosen[:, None] == jnp.arange(EXPERTS, dtype=jnp.int32)[None, :]).astype(jnp.int32)
    earlier = jnp.cumsum(one_hot, axis=0) - one_hot
    slot = jnp.sum(earlier * one_hot, axis=1) - core.astype(jnp.int32) * slots
    position = jnp.where((slot >= 0) & (slot < slots), chosen * capacity + slot, -capacity)
    position = position.reshape(tok_rows, 2)
    columns = jnp.arange(EXPERTS * capacity, dtype=jnp.int32)

    def matches(part):
        return (position + part * slots)[:, :, None] == columns[None, None, :]

    select = jnp.concatenate(
        [jnp.sum(matches(p).astype(jnp.float32), axis=1) for p in (0, 1)]
    ).astype(jnp.bfloat16)
    weighing = jnp.concatenate(
        [jnp.sum(matches(p).astype(jnp.float32) * route_weights[:, :, None], axis=1) for p in (0, 1)]
    )
    mine = lax.dynamic_slice_in_dim(hidden_states, x_index * width, width, 1)
    mine = jnp.concatenate([mine[:, :narrow], mine[:, narrow:]], axis=0)
    packed = jnp.einsum("tj,td->jd", select, mine, preferred_element_type=jnp.float32)
    packed = packed.astype(jnp.bfloat16).reshape(EXPERTS, capacity, narrow)

    arrived = lax.all_to_all(packed, ("y", "zhi"), 0, 0, tiled=True)
    rows = EXPERTS * slots
    half = rows // 2
    arrived = jnp.swapaxes(arrived.reshape(EXPERTS, 2, slots, narrow), 1, 2).reshape(rows, width)

    blocks = {0: arrived}
    for k in (1, 3, 2):
        blocks[k] = shifted(arrived, "zlo", MEMBERS, k)

    pieces = {}
    for k in (0, 1, 3, 2):
        own = blocks[k]
        plus, minus = shifted(own, "x", X, 1), shifted(own, "x", X, -1)
        far0 = shifted(plus[:half], "x", X, 1)
        far1 = shifted(minus[half:], "x", X, -1)
        pieces[k] = (own, plus, minus, far0, far1)

    x_at = x_index.astype(jnp.int32).reshape(1)
    partial = {}
    for chunk in CHUNKS:
        for k, out in zip(chunk, ffn(x_at, [pieces[k] for k in chunk], weights)):
            partial[k] = out

    sums = []
    for k in (1, 3, 2, 0):
        far0, far1, plus0, plus1, minus0, minus1, own = partial[k]
        l1 = shifted(far0, "x", X, 1)
        r1 = shifted(far1, "x", X, -1)
        l3 = shifted(minus1, "x", X, 1)
        r3 = shifted(plus0, "x", X, -1)
        l2 = shifted(add(minus0, l1), "x", X, 1)
        r2 = shifted(add(plus1, r1), "x", X, -1)
        done = jnp.concatenate([add(own[:half], r3, l2), add(own[half:], l3, r2)], axis=0)
        sums.append(done if k == 0 else shifted(done, "zlo", MEMBERS, -k))
    summed = add(*sums)

    outgoing = jnp.swapaxes(summed.reshape(EXPERTS, slots, 2, narrow), 1, 2)
    returned = lax.all_to_all(
        outgoing.reshape(EXPERTS, capacity, narrow), ("y", "zhi"), 0, 0, tiled=True
    )
    contribution = jnp.dot(
        weighing,
        returned.reshape(EXPERTS * capacity, narrow),
        preferred_element_type=jnp.float32,
    )
    parts = contribution[:tok_rows], contribution[tok_rows:]
    kept = jnp.where(core == 0, parts[0], parts[1])
    given = jnp.where(core == 0, parts[1], parts[0]).astype(jnp.bfloat16)
    return (kept + shifted(given, "core", 2, 1).astype(jnp.float32)).astype(jnp.bfloat16)


def solution(mesh):
    fine = Mesh(mesh.devices.reshape(X, 2, 4, 2, MEMBERS), ("x", "core", "y", "zhi", "zlo"))
    ep, section = ("y", "zhi", "zlo"), ("x", "core")
    return jax.shard_map(
        on_device,
        mesh=fine,
        in_specs=(
            P(ep, None),
            P(ep, None),
            P(ep, None),
            P(ep, None, section),
            P(ep, None, section),
            P(ep, section, None),
        ),
        out_specs=P(ep, section),
        check_vma=False,
    )
```

```python
import functools

import jax
import jax.numpy as jnp
from jax import lax
from jax.experimental import pallas as pl
from jax.experimental.pallas import tpu as pltpu
from jax.sharding import Mesh
from jax.sharding import PartitionSpec as P

EXPERTS = 8
MEMBERS = 4
X = 4
CHUNKS = ((0, 1, 3), (2,))
FAR = {0: 1, 1: -1, 3: 1, 2: -1}
GATE_ORDER = (0, 1, 3, 2)
DOWN_ORDER = (2, 1, 3, 0)


def shifted(v, axis, n, step):
    return lax.ppermute(v, axis, [((i + step) % n, i) for i in range(n)])


def quarter_of(order, x, step):
    rel = jnp.int32(order[0])
    for i in range(1, 4):
        rel = jnp.where(step == i, order[i], rel)
    return lax.rem(x + rel, 4)


def ffn_kernel(blocks, rows, x_ref, *refs):
    pieces = [refs[4 * b : 4 * b + 4] for b in range(blocks)]
    refs = refs[4 * blocks :]
    gates_ups, downs = refs[:4], refs[4:6]
    outs = [refs[6 + 4 * b : 10 + 4 * b] for b in range(blocks)]
    rows_x, wide, tall, acc, hid, res, wide_sem, tall_sem = refs[6 + 4 * blocks :]
    width = rows_x.shape[2]
    hidden = hid.shape[1] // 2
    x = x_ref[0]

    def gate_copies(step, slot):
        at = pl.ds(pl.multiple_of(quarter_of(GATE_ORDER, x, step) * width, width), width)
        return [
            pltpu.make_async_copy(
                w.at[at, :], wide.at[slot, :, pl.ds(i * hidden, hidden)], wide_sem.at[slot, i]
            )
            for i, w in enumerate(gates_ups)
        ]

    def down_copies(step, slot):
        at = pl.ds(pl.multiple_of(quarter_of(DOWN_ORDER, x, step) * width, width), width)
        return [
            pltpu.make_async_copy(
                w.at[:, at], tall.at[slot, pl.ds(i * hidden, hidden), :], tall_sem.at[slot, i]
            )
            for i, w in enumerate(downs)
        ]

    for copies in (gate_copies, down_copies):
        for slot in (0, 1):
            for copy in copies(jnp.int32(slot), slot):
                copy.start()

    for b in range(blocks):
        for at, piece in enumerate(pieces[b]):
            rows_x[at, b * rows : (b + 1) * rows, :] = piece[...]
    acc[...] = jnp.zeros_like(acc)

    def gate_step(step, carry):
        slot = lax.rem(step, 2)
        for copy in gate_copies(step, slot):
            copy.wait()
        acc[...] += jnp.dot(rows_x[step], wide[slot], preferred_element_type=jnp.float32)

        @pl.when(step < 2)
        def _():
            for copy in gate_copies(step + 2, slot):
                copy.start()

        return carry

    lax.fori_loop(0, 4, gate_step, 0)
    gate = acc[:, : 2 * hidden]
    hid[...] = (gate / (1.0 + jnp.exp(-gate)) * acc[:, 2 * hidden :]).astype(jnp.bfloat16)

    def down_step(step, carry):
        slot = lax.rem(step, 2)
        for copy in down_copies(step, slot):
            copy.wait()
        out = jnp.dot(hid[...], tall[slot], preferred_element_type=jnp.float32)
        res[step] = out.astype(jnp.bfloat16)

        @pl.when(step < 2)
        def _():
            for copy in down_copies(step + 2, slot):
                copy.start()

        return carry

    lax.fori_loop(0, 4, down_step, 0)
    for b in range(blocks):
        for at, out in enumerate(outs[b]):
            out[...] = res[at, b * rows : (b + 1) * rows, :]


def ffn(x_at, pieces, weights):
    blocks = len(pieces)
    rows, width = pieces[0][0].shape
    hidden = weights[0].shape[1]
    total = blocks * rows
    vmem = pl.BlockSpec(memory_space=pltpu.VMEM)
    flat = [p for block in pieces for p in block]
    outs = pl.pallas_call(
        functools.partial(ffn_kernel, blocks, rows),
        in_specs=[pl.BlockSpec(memory_space=pltpu.SMEM)]
        + [vmem] * len(flat)
        + [pl.BlockSpec(memory_space=pltpu.HBM)] * 6,
        out_specs=[vmem] * len(flat),
        out_shape=[jax.ShapeDtypeStruct((rows, width), jnp.bfloat16)] * len(flat),
        scratch_shapes=[
            pltpu.VMEM((4, total, width), jnp.bfloat16),
            pltpu.VMEM((2, width, 4 * hidden), jnp.bfloat16),
            pltpu.VMEM((2, 2 * hidden, width), jnp.bfloat16),
            pltpu.VMEM((total, 4 * hidden), jnp.float32),
            pltpu.VMEM((total, 2 * hidden), jnp.bfloat16),
            pltpu.VMEM((4, total, width), jnp.bfloat16),
            pltpu.SemaphoreType.DMA((2, 4)),
            pltpu.SemaphoreType.DMA((2, 2)),
        ],
        compiler_params=pltpu.CompilerParams(vmem_limit_bytes=30 << 20),
        cost_estimate=pl.CostEstimate(
            flops=2 * total * 4 * width * 2 * hidden * 3,
            bytes_accessed=6 * 4 * width * hidden * 2 + 2 * total * 4 * width * 2,
            transcendentals=total * 2 * hidden,
        ),
        name="ffn",
    )(x_at, *flat, *[pltpu.with_memory_space_constraint(w, pltpu.HBM) for w in weights])
    return [outs[4 * b : 4 * b + 4] for b in range(blocks)]


def add(*parts):
    return functools.reduce(jnp.add, [p.astype(jnp.float32) for p in parts]).astype(jnp.bfloat16)


def on_device(hidden_states, route_experts, route_weights, gate_weight, up_weight, down_weight):
    x_index, core = lax.axis_index("x"), lax.axis_index("core")
    tok_rows, features = hidden_states.shape
    capacity = tok_rows // 2
    slots = capacity // 2
    width = features // X
    narrow = width // 2

    chosen = route_experts.reshape(-1)
    one_hot = (chosen[:, None] == jnp.arange(EXPERTS, dtype=jnp.int32)[None, :]).astype(jnp.int32)
    earlier = jnp.cumsum(one_hot, axis=0) - one_hot
    slot = jnp.sum(earlier * one_hot, axis=1) - core.astype(jnp.int32) * slots
    position = jnp.where((slot >= 0) & (slot < slots), chosen * capacity + slot, -capacity)
    position = position.reshape(tok_rows, 2)
    columns = jnp.arange(EXPERTS * capacity, dtype=jnp.int32)

    def matches(part):
        return (position + part * slots)[:, :, None] == columns[None, None, :]

    select = jnp.concatenate(
        [jnp.sum(matches(p).astype(jnp.float32), axis=1) for p in (0, 1)]
    ).astype(jnp.bfloat16)
    weighing = jnp.concatenate(
        [jnp.sum(matches(p).astype(jnp.float32) * route_weights[:, :, None], axis=1) for p in (0, 1)]
    )
    mine = lax.dynamic_slice_in_dim(hidden_states, x_index * width, width, 1)
    mine = jnp.concatenate([mine[:, :narrow], mine[:, narrow:]], axis=0)
    packed = jnp.einsum("tj,td->jd", select, mine, preferred_element_type=jnp.float32)
    packed = packed.astype(jnp.bfloat16).reshape(EXPERTS, capacity, narrow)

    arrived = lax.all_to_all(packed, ("y", "zhi"), 0, 0, tiled=True)
    rows = EXPERTS * slots
    arrived = jnp.swapaxes(arrived.reshape(EXPERTS, 2, slots, narrow), 1, 2).reshape(rows, width)

    own_w = (gate_weight[0], up_weight[0], down_weight[0])
    arrived, *sent_w = lax.optimization_barrier((arrived, *own_w))
    other_w = [shifted(w, "core", 2, 1) for w in sent_w]
    weights = [own_w[0], other_w[0], own_w[1], other_w[1], own_w[2], other_w[2]]

    blocks = {0: arrived}
    for k in (1, 3, 2):
        blocks[k] = shifted(arrived, "zlo", MEMBERS, k)

    pieces = {}
    for k in (0, 1, 3, 2):
        own = blocks[k]
        plus, minus = shifted(own, "x", X, 1), shifted(own, "x", X, -1)
        far = shifted({1: plus, -1: minus}[FAR[k]], "x", X, FAR[k])
        pieces[k] = (own, plus, minus, far)

    x_at = x_index.astype(jnp.int32).reshape(1)
    partial = {}
    for chunk in CHUNKS:
        for k, out in zip(chunk, ffn(x_at, [pieces[k] for k in chunk], weights)):
            partial[k] = out

    sums = []
    for k in (1, 3, 2, 0):
        far, plus, minus, own = partial[k]
        way = -FAR[k]
        first = shifted(far, "x", X, way)
        relay, direct = (minus, plus) if way == 1 else (plus, minus)
        direct = shifted(direct, "x", X, -way)
        relay = shifted(add(relay, first), "x", X, way)
        done = add(own, direct, relay)
        sums.append(done if k == 0 else shifted(done, "zlo", MEMBERS, -k))
    summed = add(*sums)

    outgoing = jnp.swapaxes(summed.reshape(EXPERTS, slots, 2, narrow), 1, 2)
    returned = lax.all_to_all(
        outgoing.reshape(EXPERTS, capacity, narrow), ("y", "zhi"), 0, 0, tiled=True
    )
    contribution = jnp.dot(
        weighing,
        returned.reshape(EXPERTS * capacity, narrow),
        preferred_element_type=jnp.float32,
    )
    parts = contribution[:tok_rows], contribution[tok_rows:]
    kept = jnp.where(core == 0, parts[0], parts[1])
    given = jnp.where(core == 0, parts[1], parts[0]).astype(jnp.bfloat16)
    return (kept + shifted(given, "core", 2, 1).astype(jnp.float32)).astype(jnp.bfloat16)


def solution(mesh):
    fine = Mesh(mesh.devices.reshape(X, 2, 4, 2, MEMBERS), ("x", "core", "y", "zhi", "zlo"))
    ep, section = ("y", "zhi", "zlo"), ("x", "core")
    return jax.shard_map(
        on_device,
        mesh=fine,
        in_specs=(
            P(ep, None),
            P(ep, None),
            P(ep, None),
            P(ep, None, section),
            P(ep, None, section),
            P(ep, section, None),
        ),
        out_specs=P(ep, section),
        check_vma=False,
    )
```
